32 devices in a mesh: aux: 8 (over z, x), lmo: 4 (over y, core).
Axes of the slice: x: 2, y: 2, z: 4, core: 2. Of those that a mesh axis runs over, the one named last changes fastest.
Arguments:
- aux_ints: bfloat16 [256, 768, 768], P(('aux', 'lmo')), may hold values from -6 to 6
- lmo_coef: bfloat16 [128, 384], P(('aux', 'lmo')), may hold values from -0.3125 to 0.3125
- ao_domain: int32 [128, 3], replicated, may hold values from 0 to 5, as said below
- ao_count: int32 [128], replicated, may hold values from 1 to 3
- pao_domain: int32 [128, 3], replicated, may hold values from 0 to 5, as said below
- pao_count: int32 [128], replicated, may hold values from 1 to 3, as said below
- owner_order: int32 [128], replicated, may hold values from 0 to 127, as said below
- pao_coef: bfloat16 [128, 384, 256], P(('aux', 'lmo')), may hold values from -0.3125 to 0.3125
Outputs:
- pair_ints: bfloat16 [128, 256, 256], P(('aux', 'lmo'))
- pair_metric: float32 [128, 256, 256], P(('aux', 'lmo'))
The draws below stay inside these ranges and needn't reach their ends.
Inputs may be any that keep to these rules, and one draw needn't show every extreme that they name: `ao_domain`: each row holds 3 different block numbers; slots from ao_count on are unused. `pao_domain`: each row holds 3 different block numbers; slots from pao_count on are unused. `pao_count`: the LMOs of the 4 owner slots of one device use together at most 8 PAO block slots, and those of some device use exactly 8. `owner_order`: every LMO stands in exactly one slot.
All inputs are finite; a program needn't handle non-finite values.
Results may differ from the reference program's by a relative error of at most 0.0049.
Values may be sent and summed in bfloat16 or wider, within the bound.
A program may use at most 128 MiB of HBM per device.

```python
import jax
import jax.numpy as jnp
from jax import lax

BLK = 128
NBA = 6
DB = 3
PB = 3
NPAO = 256
P_D = 8
LMO_DEV = 4
AO = 768
NAUX = 256
NLMO = 128
USED = 8


def draw_rows(key, row_depth):
    subkeys = jax.random.split(key, NLMO)

    def one_row(subkey):
        return jax.random.permutation(subkey, NBA)[:row_depth]
    return jax.vmap(one_row)(subkeys).astype(jnp.int32)


def draw_ao_domain(key, part):
    return draw_rows(jax.random.fold_in(key, 11), DB)


def draw_pao_domain(key, part):
    return draw_rows(jax.random.fold_in(key, 23), PB)


def owner_tables(key):
    base = jax.random.fold_in(key, 31)
    order_key, target_key, full_key, unit_key = jax.random.split(base, 4)
    order = jax.random.permutation(order_key, NLMO).astype(jnp.int32)
    groups = NLMO // LMO_DEV
    target = jax.random.randint(target_key, (groups,), LMO_DEV, USED + 1).astype(jnp.int32)
    full_group = jax.random.randint(full_key, (), 0, groups).astype(jnp.int32)
    target = jnp.where(jnp.arange(groups, dtype=jnp.int32) == full_group, USED, target)
    counts = jnp.ones((groups, LMO_DEV), jnp.int32)
    members = jnp.arange(LMO_DEV, dtype=jnp.int32)
    for unit in range(USED - LMO_DEV):
        scores = jax.random.randint(jax.random.fold_in(unit_key, unit), (groups, LMO_DEV), 0, 1 << 20).astype(jnp.int32)
        scores = scores * LMO_DEV + members[None, :]
        scores = jnp.where(counts < PB, scores, -1)
        picked = jnp.argmax(scores, axis=1).astype(jnp.int32)
        adding = (members[None, :] == picked[:, None]) & (unit < target - LMO_DEV)[:, None]
        counts = counts + adding.astype(jnp.int32)
    by_slot = counts.reshape(NLMO)
    pao_count = jnp.zeros((NLMO,), jnp.int32).at[order].set(by_slot)
    return (order, pao_count)


def draw_owner_order(key, part):
    return owner_tables(key)[0]


def draw_pao_count(key, part):
    return owner_tables(key)[1]


def set_ends(entries, stream_key, low, high):
    longest = entries.shape.index(max(entries.shape))
    spots = []
    for shift in (0, 1):
        where = [jax.random.randint(jax.random.fold_in(stream_key, axis), (), 0, length) for axis, length in enumerate(entries.shape)]
        where[longest] = (where[longest] + shift) % entries.shape[longest]
        spots.append(tuple(where))
    return entries.at[spots[0]].set(low).at[spots[1]].set(high)


def shard_levels(stream_key, shape, shards, least, high):
    factor_of, own = 1.0, jax.random.fold_in(stream_key, 6)
    for position, shards_of in shards:
        steps = jnp.exp(jax.random.uniform(jax.random.fold_in(own, position), (shards_of,), jnp.float32, least / len(shards), high / len(shards)))
        factor_of = factor_of * jnp.repeat(steps, shape[position] // shards_of).reshape([-1 if axis == position else 1 for axis in range(len(shape))])
    return factor_of


def gaussian(stream_key, dims, spread, reach, cuts=(), kind=jnp.bfloat16):
    values = jax.random.normal(stream_key, dims, jnp.float32) * spread
    if len(cuts) > 0:
        values = shard_levels(stream_key, dims, cuts, -0.22, 0.18) * values
    return jnp.clip(values, min=-reach, max=reach).astype(kind)


def setup_inputs(seed: int = 0) -> dict:
    streams_of = jax.random.split(jax.random.key(seed), 9)
    aux_ints = gaussian(streams_of[0], (NAUX, AO, AO), 1.0, 6.0, ((0, 32),))
    lmo_coef = gaussian(streams_of[1], (NLMO, DB * BLK), (DB * BLK) ** -0.5, 0.3125, ((0, 32),))
    ao_domain = draw_ao_domain(jax.random.fold_in(streams_of[8], 71), 0)
    ao_count = set_ends(jax.random.randint(streams_of[3], (NLMO,), 1, DB + 1), jax.random.fold_in(streams_of[3], 1), 1, DB).astype(jnp.int32)
    pao_domain = draw_pao_domain(jax.random.fold_in(streams_of[8], 71), 0)
    pao_count = draw_pao_count(jax.random.fold_in(streams_of[8], 71), 0)
    owner_order = draw_owner_order(jax.random.fold_in(streams_of[8], 71), 0)
    pao_coef = gaussian(streams_of[7], (NLMO, PB * BLK, NPAO), (PB * BLK) ** -0.5, 0.3125, ((0, 32),))
    return dict(aux_ints=aux_ints, lmo_coef=lmo_coef, ao_domain=ao_domain, ao_count=ao_count, pao_domain=pao_domain, pao_count=pao_count, owner_order=owner_order, pao_coef=pao_coef)


def place(lmo_coef, domain, block_count, blocks):
    lmo_total = lmo_coef.shape[0]
    in_domain = jnp.arange(DB)[None, :] < block_count[:, None]
    onehot = ((domain[:, :, None] == jnp.arange(blocks)[None, None, :]) & in_domain[:, :, None]).astype(jnp.float32)
    tiles = lmo_coef.astype(jnp.float32).reshape(lmo_total, DB, BLK)
    dense_coef = jnp.einsum("ikb,ikn->bni", onehot, tiles, precision=lax.Precision.HIGHEST)
    return dense_coef.reshape(blocks * BLK, lmo_total).astype(jnp.bfloat16)


def select(half_ints, domain, block_count, blocks):
    row_total = half_ints.shape[0]
    lmo_total = half_ints.shape[2]
    in_domain = jnp.arange(PB)[None, :] < block_count[:, None]
    onehot = ((domain[:, :, None] == jnp.arange(blocks)[None, None, :]) & in_domain[:, :, None]).astype(jnp.float32)
    tiled = half_ints.reshape(row_total, blocks, BLK, lmo_total)
    picked = jnp.einsum("pbni,ikb->ipkn", tiled, onehot, precision=lax.Precision.HIGHEST)
    return picked.reshape(lmo_total, row_total, PB * BLK).astype(jnp.bfloat16)


def reference(aux_ints, lmo_coef, ao_domain, ao_count, pao_domain, pao_count, owner_order, pao_coef):
    blocks = aux_ints.shape[1] // BLK
    dense_coef = place(lmo_coef, ao_domain, ao_count, blocks)

    def transform(block_ints):
        row_total = block_ints.shape[0]
        half_ints = jnp.dot(block_ints.reshape(row_total * AO, AO), dense_coef,
                            preferred_element_type=jnp.float32).reshape(row_total, AO, -1)
        return select(half_ints, pao_domain, pao_count, blocks)

    stacked = lax.map(transform, aux_ints.reshape(NAUX // P_D, P_D, AO, AO))
    selected = jnp.transpose(stacked, (1, 0, 2, 3)).reshape(NLMO, NAUX, PB * BLK)
    ordered = selected[owner_order]

    def per_slot(operands):
        rows_here, coef_here = operands
        pair_row = jnp.dot(rows_here, coef_here, preferred_element_type=jnp.float32).astype(jnp.bfloat16)
        wide_row = pair_row.astype(jnp.float32)
        metric_row = jnp.dot(wide_row.T, wide_row, precision=lax.Precision.HIGHEST) / NAUX
        return pair_row, metric_row

    pair_ints, pair_metric = lax.map(per_slot, (ordered, pao_coef))
    return pair_ints, pair_metric
```

```python
import functools

import jax
import jax.numpy as jnp
from jax import lax
from jax.experimental import pallas as pl
from jax.experimental.pallas import tpu as pltpu
from jax.sharding import PartitionSpec as P

BLK = 128
DB = 3
PB = 3
USED = 8
MESH = pl.DeviceIdType.MESH


def exchange(
    n_aux, n_lmo,
    aux_hbm, lmo_ref, ao_dom, ao_cnt, pao_dom, pao_cnt, order, recv,
    aux, coef_all, coef32, dense, half, tab, send,
    aux_sem, coef_send, coef_recv, out_send, out_recv, own_sem,
):
    dev = n_aux * n_lmo
    rows, ao, _ = aux_hbm.shape
    blocks = ao // BLK
    per = lmo_ref.shape[0]
    lmos = per * dev
    me = lax.axis_index("aux") * n_lmo + lax.axis_index("lmo")

    def coords(d):
        return (d // n_lmo, lax.rem(d, n_lmo))

    def partner(t):
        return lax.rem(me + t, dev)

    def load(p):
        return pltpu.make_async_copy(aux_hbm.at[p], aux.at[p], aux_sem.at[p])

    for p in range(rows):
        load(p).start()

    barrier = pltpu.get_barrier_semaphore()

    @pl.loop(1, dev)
    def _(t):
        pl.semaphore_signal(barrier, inc=1, device_id=coords(partner(t)), device_id_type=MESH)

    pl.semaphore_wait(barrier, dev - 1)

    def coef_copy(slot, d):
        return pltpu.make_async_remote_copy(
            src_ref=lmo_ref, dst_ref=coef_all.at[slot],
            send_sem=coef_send.at[d], recv_sem=coef_recv.at[slot],
            device_id=coords(d), device_id_type=MESH,
        )

    @pl.loop(1, dev)
    def _(t):
        coef_copy(me, partner(t)).start()

    coef_all[me] = lmo_ref[...]

    @pl.loop(0, dev)
    def _(d):
        lmo = [order[d * per + j] for j in range(per)]
        cnt = [pao_cnt[i] for i in lmo]
        for s in range(USED):
            i, k = lmo[0], jnp.int32(s)
            start = jnp.int32(0)
            for j in range(1, per):
                start = start + cnt[j - 1]
                past = s >= start
                i = jnp.where(past, lmo[j], i)
                k = jnp.where(past, s - start, k)
            tab[d * USED + s] = i * blocks + pao_dom[jnp.minimum(k, PB - 1), i]

    @pl.loop(1, dev)
    def _(t):
        d = partner(t)
        coef_copy(d, d).wait_recv()

    for d in range(dev):
        coef32[d * per:(d + 1) * per, :] = coef_all[d].astype(jnp.float32)

    eye = lax.broadcasted_iota(jnp.int32, (lmos, lmos), 0) == lax.broadcasted_iota(
        jnp.int32, (lmos, lmos), 1
    )
    where_to = []
    for k in range(DB):
        block = jnp.where(ao_cnt[...] > k, ao_dom[k:k + 1, :], -1).astype(jnp.float32)
        column = jnp.sum(jnp.where(eye, block, 0.0), axis=1, keepdims=True)
        where_to.append(jnp.broadcast_to(column, (lmos, BLK)))
    for b in range(blocks):
        total = jnp.zeros((lmos, BLK), jnp.float32)
        for k in range(DB):
            total = jnp.where(where_to[k] == b, coef32[:, k * BLK:(k + 1) * BLK], total)
        dense[:, b * BLK:(b + 1) * BLK] = total.astype(jnp.bfloat16)

    wide = 2 * BLK
    flat = half.reshape(lmos * blocks * rows, BLK)
    for p in range(rows):
        load(p).wait()
        for c in range(ao // wide):
            out = lax.dot_general(
                dense[...], aux[p, c * wide:(c + 1) * wide, :],
                (((1,), (1,)), ((), ())), preferred_element_type=jnp.float32,
            )
            for h in range(2):
                b = c * 2 + h
                flat[pl.ds(b * rows + p, lmos, stride=blocks * rows), :] = (
                    out[:, h * BLK:(h + 1) * BLK]
                )

    def pack(d):
        for s in range(USED):
            row = tab[d * USED + s]
            send[d, s] = half[row].astype(jnp.bfloat16)

    def out_copy(slot, d):
        return pltpu.make_async_remote_copy(
            src_ref=send.at[d], dst_ref=recv.at[slot],
            send_sem=out_send.at[d], recv_sem=out_recv.at[slot],
            device_id=coords(d), device_id_type=MESH,
        )

    pack(partner(1))

    @pl.loop(1, dev)
    def _(t):
        pack(partner(t + 1))
        out_copy(me, partner(t)).start()

    own = pltpu.make_async_copy(send.at[me], recv.at[me], own_sem)
    own.start()

    @pl.loop(1, dev)
    def _(t):
        d = partner(t)
        coef_copy(d, d).wait_send()
        out_copy(d, d).wait_send()
        out_copy(d, d).wait_recv()

    own.wait()


def contract(n_lmo, per, recv, coef, pao_cnt, order, pair, metric, kept):
    g = pl.program_id(0)
    me = lax.axis_index("aux") * n_lmo + lax.axis_index("lmo")
    dev, _, rows, _ = recv.shape
    start = jnp.int32(0)
    for j in range(per - 1):
        start = start + jnp.where(j < g, pao_cnt[order[me * per + j]], 0)
    count = pao_cnt[order[me * per + g]]
    for k in range(PB):
        slot = jnp.minimum(start + k, USED - 1)
        tile = recv[:, slot].astype(jnp.float32).reshape(dev * rows, BLK)
        tile = jnp.where(k < count, tile, 0.0)
        kept[:, k * BLK:(k + 1) * BLK] = tile.astype(jnp.bfloat16)
    row = jnp.dot(kept[...], coef[0], preferred_element_type=jnp.float32).astype(jnp.bfloat16)
    pair[0] = row
    metric[0] = lax.dot_general(
        row, row, (((0,), (0,)), ((), ())), preferred_element_type=jnp.float32
    ) / (dev * rows)


def shards(mesh, aux_ints, lmo_coef, ao_domain, ao_count, pao_domain, pao_count, owner_order, pao_coef):
    n_aux, n_lmo = mesh.shape["aux"], mesh.shape["lmo"]
    dev = n_aux * n_lmo
    rows, ao, _ = aux_ints.shape
    blocks = ao // BLK
    per = lmo_coef.shape[0]
    lmos = per * dev
    npao = pao_coef.shape[2]
    vmem = pl.BlockSpec(memory_space=pltpu.VMEM)
    smem = pl.BlockSpec(memory_space=pltpu.SMEM)
    anywhere = pl.BlockSpec(memory_space=pl.ANY)
    recv = pl.pallas_call(
        functools.partial(exchange, n_aux, n_lmo),
        out_shape=jax.ShapeDtypeStruct((dev, USED, rows, BLK), jnp.bfloat16),
        in_specs=[anywhere, vmem, vmem, vmem, smem, smem, smem],
        out_specs=anywhere,
        scratch_shapes=[
            pltpu.VMEM((rows, ao, ao), jnp.bfloat16),
            pltpu.VMEM((dev, per, DB * BLK), jnp.bfloat16),
            pltpu.VMEM((lmos, DB * BLK), jnp.float32),
            pltpu.VMEM((lmos, ao), jnp.bfloat16),
            pltpu.VMEM((lmos * blocks, rows, BLK), jnp.float32),
            pltpu.SMEM((dev * USED,), jnp.int32),
            pltpu.VMEM((dev, USED, rows, BLK), jnp.bfloat16),
            pltpu.SemaphoreType.DMA((rows,)),
            pltpu.SemaphoreType.DMA((dev,)),
            pltpu.SemaphoreType.DMA((dev,)),
            pltpu.SemaphoreType.DMA((dev,)),
            pltpu.SemaphoreType.DMA((dev,)),
            pltpu.SemaphoreType.DMA,
        ],
        compiler_params=pltpu.CompilerParams(
            collective_id=0, has_side_effects=True, vmem_limit_bytes=60 * 2**20
        ),
        name="exchange",
    )(aux_ints, lmo_coef, ao_domain.T, ao_count.reshape(1, lmos), pao_domain.T, pao_count, owner_order)
    pair, metric = pl.pallas_call(
        functools.partial(contract, n_lmo, per),
        grid=(per,),
        out_shape=(
            jax.ShapeDtypeStruct((per, dev * rows, npao), jnp.bfloat16),
            jax.ShapeDtypeStruct((per, npao, npao), jnp.float32),
        ),
        in_specs=[
            pl.BlockSpec((dev, USED, rows, BLK), lambda g: (0, 0, 0, 0)),
            pl.BlockSpec((1, PB * BLK, npao), lambda g: (g, 0, 0)),
            smem,
            smem,
        ],
        out_specs=(
            pl.BlockSpec((1, dev * rows, npao), lambda g: (g, 0, 0)),
            pl.BlockSpec((1, npao, npao), lambda g: (g, 0, 0)),
        ),
        scratch_shapes=[pltpu.VMEM((dev * rows, PB * BLK), jnp.bfloat16)],
        name="contract",
    )(recv, pao_coef, pao_count, owner_order)
    return pair, metric


def solution(mesh):
    split = ("aux", "lmo")
    placed = (P(split, None, None), P(split, None), P(), P(), P(), P(), P(), P(split, None, None))
    return jax.shard_map(
        functools.partial(shards, mesh),
        mesh=mesh,
        in_specs=placed,
        out_specs=(P(split, None, None), P(split, None, None)),
        check_vma=False,
    )
```

```python
import functools

import jax
import jax.numpy as jnp
from jax import lax
from jax.experimental import pallas as pl
from jax.experimental.pallas import tpu as pltpu
from jax.sharding import PartitionSpec as P

BLK = 128
DB = 3
PB = 3
PARTS = 1
USED = 8
MESH = pl.DeviceIdType.MESH


def exchange(
    n_aux, n_lmo,
    aux_hbm, lmo_ref, ao_dom, ao_cnt, pao_dom, pao_cnt, order, recv,
    aux, coef_all, coef32, dense, half, tab, send,
    aux_sem, coef_send, coef_recv, out_send, out_recv, own_sem,
):
    dev = n_aux * n_lmo
    rows, ao, _ = aux_hbm.shape
    blocks = ao // BLK
    per = lmo_ref.shape[0]
    lmos = per * dev
    me = lax.axis_index("aux") * n_lmo + lax.axis_index("lmo")

    def coords(d):
        return (d // n_lmo, lax.rem(d, n_lmo))

    def partner(t):
        return lax.rem(me + t, dev)

    def load(p):
        return pltpu.make_async_copy(aux_hbm.at[p], aux.at[p], aux_sem.at[p])

    for p in range(rows):
        load(p).start()

    barrier = pltpu.get_barrier_semaphore()

    @pl.loop(1, dev)
    def _(t):
        pl.semaphore_signal(barrier, inc=1, device_id=coords(partner(t)), device_id_type=MESH)

    pl.semaphore_wait(barrier, dev - 1)

    def coef_copy(slot, d):
        return pltpu.make_async_remote_copy(
            src_ref=lmo_ref, dst_ref=coef_all.at[slot],
            send_sem=coef_send.at[d], recv_sem=coef_recv.at[slot],
            device_id=coords(d), device_id_type=MESH,
        )

    @pl.loop(1, dev)
    def _(t):
        coef_copy(me, partner(t)).start()

    coef_all[me] = lmo_ref[...]

    @pl.loop(0, dev)
    def _(d):
        lmo = [order[d * per + j] for j in range(per)]
        cnt = [pao_cnt[i] for i in lmo]
        for s in range(USED):
            i, k = lmo[0], jnp.int32(s)
            start = jnp.int32(0)
            for j in range(1, per):
                start = start + cnt[j - 1]
                past = s >= start
                i = jnp.where(past, lmo[j], i)
                k = jnp.where(past, s - start, k)
            tab[d * USED + s] = i * blocks + pao_dom[jnp.minimum(k, PB - 1), i]

    @pl.loop(1, dev)
    def _(t):
        d = partner(t)
        coef_copy(d, d).wait_recv()

    for d in range(dev):
        coef32[d * per:(d + 1) * per, :] = coef_all[d].astype(jnp.float32)

    eye = lax.broadcasted_iota(jnp.int32, (lmos, lmos), 0) == lax.broadcasted_iota(
        jnp.int32, (lmos, lmos), 1
    )
    where_to = []
    for k in range(DB):
        block = jnp.where(ao_cnt[...] > k, ao_dom[k:k + 1, :], -1).astype(jnp.float32)
        column = jnp.sum(jnp.where(eye, block, 0.0), axis=1, keepdims=True)
        where_to.append(jnp.broadcast_to(column, (lmos, BLK)))
    for b in range(blocks):
        total = jnp.zeros((lmos, BLK), jnp.float32)
        for k in range(DB):
            total = jnp.where(where_to[k] == b, coef32[:, k * BLK:(k + 1) * BLK], total)
        dense[:, b * BLK:(b + 1) * BLK] = total.astype(jnp.bfloat16)

    flat = half.reshape(lmos * blocks * rows, BLK)
    chunk = rows // PARTS

    def transform(g):
        for p in range(g * chunk, (g + 1) * chunk):
            load(p).wait()
        out = lax.dot_general(
            dense[...], aux[g * chunk:(g + 1) * chunk].reshape(chunk * ao, ao),
            (((1,), (1,)), ((), ())), preferred_element_type=jnp.float32,
        )
        for q in range(chunk):
            for b in range(blocks):
                first = q * ao + b * BLK
                flat[pl.ds(b * rows + g * chunk + q, lmos, stride=blocks * rows), :] = (
                    out[:, first:first + BLK]
                )

    def pack(g, d):
        for s in range(USED):
            row = tab[d * USED + s]
            send[g, d, s] = half[row, g * chunk:(g + 1) * chunk, :].astype(jnp.bfloat16)

    def out_copy(g, slot, d):
        return pltpu.make_async_remote_copy(
            src_ref=send.at[g, d], dst_ref=recv.at[g, slot],
            send_sem=out_send.at[g, d], recv_sem=out_recv.at[g, slot],
            device_id=coords(d), device_id_type=MESH,
        )

    def own_copy(g):
        return pltpu.make_async_copy(send.at[g, me], recv.at[g, me], own_sem.at[g])

    for g in range(PARTS):
        transform(g)
        pack(g, partner(1))

        @pl.loop(1, dev)
        def _(t):
            pack(g, partner(t + 1))
            out_copy(g, me, partner(t)).start()

        own_copy(g).start()

    @pl.loop(1, dev)
    def _(t):
        d = partner(t)
        coef_copy(d, d).wait_send()
        for g in range(PARTS):
            out_copy(g, d, d).wait_send()
            out_copy(g, d, d).wait_recv()

    for g in range(PARTS):
        own_copy(g).wait()


def contract(n_lmo, per, recv, coef, pao_cnt, order, pair, metric, pair_out, metric_out, sem):
    me = lax.axis_index("aux") * n_lmo + lax.axis_index("lmo")
    _, dev, _, chunk, _ = recv.shape
    rows = PARTS * chunk
    start = jnp.int32(0)
    copies = []
    for g in range(per):
        count = pao_cnt[order[me * per + g]]
        tiles = []
        for k in range(PB):
            slot = jnp.minimum(start + k, USED - 1)
            tile = jnp.concatenate(
                [recv[h, :, slot].astype(jnp.float32) for h in range(PARTS)], axis=1
            ).reshape(dev * rows, BLK)
            tiles.append(jnp.where(k < count, tile, 0.0).astype(jnp.bfloat16))
        start = start + count
        row = jnp.dot(
            jnp.concatenate(tiles, axis=1), coef[g], preferred_element_type=jnp.float32
        ).astype(jnp.bfloat16)
        pair_out[g] = row
        metric_out[g] = lax.dot_general(
            row, row, (((0,), (0,)), ((), ())), preferred_element_type=jnp.float32
        ) / (dev * rows)
        for c, (src, dst) in enumerate(((pair_out, pair), (metric_out, metric))):
            copies.append(pltpu.make_async_copy(src.at[g], dst.at[g], sem.at[g, c]))
            copies[-1].start()
    for copy in copies:
        copy.wait()


def shards(mesh, aux_ints, lmo_coef, ao_domain, ao_count, pao_domain, pao_count, owner_order, pao_coef):
    n_aux, n_lmo = mesh.shape["aux"], mesh.shape["lmo"]
    dev = n_aux * n_lmo
    rows, ao, _ = aux_ints.shape
    blocks = ao // BLK
    per = lmo_coef.shape[0]
    lmos = per * dev
    npao = pao_coef.shape[2]
    vmem = pl.BlockSpec(memory_space=pltpu.VMEM)
    smem = pl.BlockSpec(memory_space=pltpu.SMEM)
    anywhere = pl.BlockSpec(memory_space=pl.ANY)
    recv = pl.pallas_call(
        functools.partial(exchange, n_aux, n_lmo),
        out_shape=jax.ShapeDtypeStruct((PARTS, dev, USED, rows // PARTS, BLK), jnp.bfloat16),
        in_specs=[anywhere, vmem, vmem, vmem, smem, smem, smem],
        out_specs=anywhere,
        scratch_shapes=[
            pltpu.VMEM((rows, ao, ao), jnp.bfloat16),
            pltpu.VMEM((dev, per, DB * BLK), jnp.bfloat16),
            pltpu.VMEM((lmos, DB * BLK), jnp.float32),
            pltpu.VMEM((lmos, ao), jnp.bfloat16),
            pltpu.VMEM((lmos * blocks, rows, BLK), jnp.float32),
            pltpu.SMEM((dev * USED,), jnp.int32),
            pltpu.VMEM((PARTS, dev, USED, rows // PARTS, BLK), jnp.bfloat16),
            pltpu.SemaphoreType.DMA((rows,)),
            pltpu.SemaphoreType.DMA((dev,)),
            pltpu.SemaphoreType.DMA((dev,)),
            pltpu.SemaphoreType.DMA((PARTS, dev)),
            pltpu.SemaphoreType.DMA((PARTS, dev)),
            pltpu.SemaphoreType.DMA((PARTS,)),
        ],
        compiler_params=pltpu.CompilerParams(
            collective_id=0, has_side_effects=True, vmem_limit_bytes=60 * 2**20
        ),
        name="exchange",
    )(aux_ints, lmo_coef, ao_domain.T, ao_count.reshape(1, lmos), pao_domain.T, pao_count, owner_order)
    pair, metric = pl.pallas_call(
        functools.partial(contract, n_lmo, per),
        out_shape=(
            jax.ShapeDtypeStruct((per, dev * rows, npao), jnp.bfloat16),
            jax.ShapeDtypeStruct((per, npao, npao), jnp.float32),
        ),
        in_specs=[
            vmem,
            vmem,
            smem,
            smem,
        ],
        out_specs=(anywhere, anywhere),
        scratch_shapes=[
            pltpu.VMEM((per, dev * rows, npao), jnp.bfloat16),
            pltpu.VMEM((per, npao, npao), jnp.float32),
            pltpu.SemaphoreType.DMA((per, 2)),
        ],
        name="contract",
    )(recv, pao_coef, pao_count, owner_order)
    return pair, metric


def solution(mesh):
    split = ("aux", "lmo")
    placed = (P(split, None, None), P(split, None), P(), P(), P(), P(), P(), P(split, None, None))
    return jax.shard_map(
        functools.partial(shards, mesh),
        mesh=mesh,
        in_specs=placed,
        out_specs=(P(split, None, None), P(split, None, None)),
        check_vma=False,
    )
```
